16 devices in a mesh: dp: 2 (over y, z), tp: 8 (over x, core).
Axes of the slice: x: 4, y: 2, z: 1, core: 2. Of those that a mesh axis runs over, the one named last changes fastest.
The devices are a block of a 4x4x4 slice.
Arguments:
- x: bfloat16 [128, 12288], P('dp'), parts along dimension 0
- k_cache: bfloat16 [128, 4096, 8, 128], P('dp', None, 'tp'), parts along dimension 0
- v_cache: bfloat16 [128, 4096, 8, 128], P('dp', None, 'tp'), parts along dimension 0
- gain_a: bfloat16 [12288], replicated
- wq: bfloat16 [12288, 12288], P(None, 'tp')
- wo: bfloat16 [12288, 12288], P('tp')
- gain_m: bfloat16 [12288], replicated
- w_gate: bfloat16 [12288, 33792], P(None, 'tp')
- w_up: bfloat16 [12288, 33792], P(None, 'tp')
- w_down: bfloat16 [33792, 12288], P('tp')
Outputs:
- output: bfloat16 [128, 12288], P('dp'), parts along dimension 0
There are 2 independent parts. The reference program is written for one: setup_inputs(seed, part) draws one part's arguments, and reference() takes and returns one part's arrays. A program takes and returns all parts, laid end to end along the dimension named above; an argument that names none is the same for every part.
All inputs are finite; a program needn't handle non-finite values.
Results may differ from the reference program's by a relative error of at most 0.017.
Values are sent between devices in bfloat16 or wider.
A program may use at most 1.5 GiB of HBM per device.

```python
import jax
import jax.numpy as jnp
from jax import lax

BATCH = 64
CACHE = 4096
D = 12288
HEADS = 96
KV_HEADS = 8
HEAD = 128
FF = 33792
THETA = 10000


def setup_inputs(seed: int = 0, part: int = 0) -> dict:
    kx, kc, kw, kn, kq, ko, km, kg, ku, kd = jax.random.split(jax.random.key(seed), 10)
    kx, kc, kw = (jax.random.fold_in(k, part) for k in (kx, kc, kw))

    def weights(key, rows, columns):
        return jax.random.normal(key, (rows, columns), jnp.float32) * rows**-0.5

    drawn = {
        "x": jax.random.normal(kx, (BATCH, D), jnp.float32),
        "k_cache": 2 * jax.random.normal(kc, (BATCH, CACHE, KV_HEADS, HEAD), jnp.float32),
        "v_cache": 4 * jax.random.normal(kw, (BATCH, CACHE, KV_HEADS, HEAD), jnp.float32),
        "gain_a": 1 + 0.1 * jax.random.normal(kn, (D,), jnp.float32),
        "wq": 2 * weights(kq, D, HEADS * HEAD),
        "wo": weights(ko, HEADS * HEAD, D),
        "gain_m": 1 + 0.1 * jax.random.normal(km, (D,), jnp.float32),
        "w_gate": weights(kg, D, FF),
        "w_up": weights(ku, D, FF),
        "w_down": 2 * weights(kd, FF, D),
    }
    return {k: v.astype(jnp.bfloat16) for k, v in drawn.items()}


def normed(x, gain):
    wide = x.astype(jnp.float32)
    scale = lax.rsqrt(jnp.mean(wide * wide, -1, keepdims=True) + 1e-6)
    return (wide * scale * gain.astype(jnp.float32)).astype(jnp.bfloat16)


def turned(t, place, theta):
    half = t.shape[-1] // 2
    angle = place.astype(jnp.float32)[:, None] * theta ** (-jnp.arange(half, dtype=jnp.float32) / half)
    cos, sin = jnp.cos(angle)[:, None], jnp.sin(angle)[:, None]
    a, b = t[..., :half].astype(jnp.float32), t[..., half:].astype(jnp.float32)
    return jnp.concatenate([a * cos - b * sin, b * cos + a * sin], -1).astype(jnp.bfloat16)


def matmul(a, w):
    return jnp.dot(a, w, preferred_element_type=jnp.float32).astype(jnp.bfloat16)


def einsum(form, a, b):
    return jnp.einsum(form, a.astype(jnp.float32), b.astype(jnp.float32))


def seen_by(a, wq, k_cache, v_cache, head, theta):
    batch, cache, kv_heads = k_cache.shape[:3]
    place = jnp.full((batch,), cache - 1)
    q = turned(matmul(a, wq).reshape(batch, -1, head), place, theta).reshape(batch, kv_heads, -1, head)
    scores = einsum("bgsd,bugd->bgsu", q, k_cache) * head**-0.5
    weights = jax.nn.softmax(scores, -1).astype(jnp.bfloat16)
    return einsum("bgsu,bugd->bgsd", weights, v_cache).astype(jnp.bfloat16).reshape(batch, -1)


def hidden_of(b, w_gate, w_up):
    gate = jnp.dot(b, w_gate, preferred_element_type=jnp.float32)
    up = jnp.dot(b, w_up, preferred_element_type=jnp.float32)
    return (jax.nn.silu(gate) * up).astype(jnp.bfloat16)


def reference(x, k_cache, v_cache, gain_a, wq, wo, gain_m, w_gate, w_up, w_down):
    seen = seen_by(normed(x, gain_a), wq, k_cache, v_cache, HEAD, THETA)
    h = (x.astype(jnp.float32) + jnp.dot(seen, wo, preferred_element_type=jnp.float32)).astype(jnp.bfloat16)
    hidden = hidden_of(normed(h, gain_m), w_gate, w_up)
    return (h.astype(jnp.float32) + jnp.dot(hidden, w_down, preferred_element_type=jnp.float32)).astype(jnp.bfloat16)
```

```python
import functools

import jax
import jax.numpy as jnp
from jax import lax
from jax.experimental import pallas as pl
from jax.experimental.pallas import tpu as pltpu
from jax.sharding import PartitionSpec as P

HEAD = 128
THETA = 10000
W = 512
SLOTS = 10
RING = 8
F32, BF16 = jnp.float32, jnp.bfloat16


def dot(a, b):
    return jnp.dot(a, b, preferred_element_type=F32)


def dot_t(a, b):
    return lax.dot_general(a, b, (((1,), (1,)), ((), ())), preferred_element_type=F32)


def kernel(
    n_tp, x_hbm, k_hbm, v_hbm, ga_hbm, wq, wo, gm_hbm, wg, wu, wd, cos_hbm, sin_hbm, o_hbm,
    slot, slot_sem, xs, hs, ys, a_ref, gains, trig, in_sem, out_sem, qacc, qf, sc, of, seen, acc, hidden,
    termf, send1, land1, own, send2, land2, rs1_s, rs1_r, rs2_s, rs2_r, ag1_s, ag1_r, ag2_s, ag2_r,
):
    d_model = x_hbm.shape[2]
    rows = x_hbm.shape[1]
    batch = x_hbm.shape[0] * rows
    cache = k_hbm.shape[1]
    attn = wq.shape[1]
    heads = attn // HEAD
    hp = qf.shape[0] // batch
    ff = wd.shape[0]
    n_k = a_ref.shape[0]
    kt = a_ref.shape[2]
    chips = n_tp // 2
    n_slots = slot.shape[0]

    me = lax.axis_index("tp")
    chip, core = lax.div(me, 2), lax.rem(me, 2)
    partner = 2 * chip + 1 - core

    def peer(d):
        return 2 * lax.rem(chip + d, chips) + core

    def source(d):
        return 2 * lax.rem(chip - d + chips, chips) + core

    barrier = pltpu.get_barrier_semaphore()
    for other in [partner] + [peer(d) for d in range(1, chips)]:
        pl.semaphore_signal(barrier, inc=1, device_id={"tp": other}, device_id_type=pl.DeviceIdType.MESH)

    n_q, n_pair, n_o = n_k * (attn // W), batch // 2, d_model // (2 * W)
    full = ff // W
    n_gu, n_d = full * 2 * n_k, d_model // W
    g_q, g_a = 0, n_q
    g_o = g_a + n_pair
    g_g = g_o + n_o
    g_r = g_g + n_gu
    g_d = g_r + 2
    g_end = g_d + n_d

    def at(i, step=W):
        return pl.ds(pl.multiple_of(i * step, step), step)

    def lane(i, width=HEAD):
        return pl.ds(i * width, width)

    def start(src, dst, s):
        pltpu.make_async_copy(src, dst, slot_sem.at[s]).start()

    def put_q(i, s):
        start(wq.at[at(lax.rem(i, n_k), kt), at(lax.div(i, n_k))], slot.at[s, pl.ds(0, kt)], s)

    def put_a(i, s):
        for j in range(2):
            start(k_hbm.at[2 * i + j], slot.at[s, pl.ds(0, cache), lane(j)], s)
            start(v_hbm.at[2 * i + j], slot.at[s, pl.ds(0, cache), lane(2 + j)], s)

    def put_o(i, s):
        for j in range(2):
            start(wo.at[:, at(2 * i + j)], slot.at[s, pl.ds(j * attn, attn)], s)

    def put_g(i, s):
        n, r = lax.div(i, 2 * n_k), lax.rem(i, 2 * n_k)

        @pl.when(r < n_k)
        def _():
            start(wg.at[at(r, kt), at(n)], slot.at[s, pl.ds(0, kt)], s)

        @pl.when(r >= n_k)
        def _():
            start(wu.at[at(r - n_k, kt), at(n)], slot.at[s, pl.ds(0, kt)], s)

    def put_r(i, s):
        def piece(w, k, j):
            start(w.at[pl.ds(k * kt, kt), pl.ds(full * W, HEAD)], slot.at[s, pl.ds(0, kt), lane(j)], s)

        @pl.when(i == 0)
        def _():
            for k in range(2):
                piece(wg, k, 2 * k)
                piece(wu, k, 2 * k + 1)

        @pl.when(i == 1)
        def _():
            piece(wg, 2, 0)
            piece(wu, 2, 1)

    def put_d(i, s):
        start(wd.at[:, at(i)], slot.at[s, pl.ds(0, ff)], s)

    parts = [(g_q, g_a, put_q), (g_a, g_o, put_a), (g_o, g_g, put_o), (g_g, g_r, put_g), (g_r, g_d, put_r), (g_d, g_end, put_d)]

    def issue(g, low, high):
        for lo, hi, put in parts:
            if lo < high and low < hi:

                @pl.when((g >= lo) & (g < hi))
                def _():
                    put(g - lo, lax.rem(g, n_slots))

    def arrived(g, height, width=W):
        s = lax.rem(g, n_slots)
        part = slot.at[s, pl.ds(0, height), pl.ds(0, width)]
        pltpu.make_async_copy(part, part, slot_sem.at[s]).wait()
        return s

    inputs = [
        pltpu.make_async_copy(x_hbm, xs, in_sem.at[0]),
        pltpu.make_async_copy(ga_hbm, gains.at[0], in_sem.at[1]),
        pltpu.make_async_copy(gm_hbm, gains.at[1], in_sem.at[2]),
        pltpu.make_async_copy(cos_hbm, trig.at[0], in_sem.at[3]),
        pltpu.make_async_copy(sin_hbm, trig.at[1], in_sem.at[4]),
    ]
    for c in inputs:
        c.start()
    for g in range(n_slots):
        issue(jnp.int32(g), g, g + 1)
    for c in inputs:
        c.wait()

    def norm_into(src, gain):
        for i in range(batch // 16):
            per = 16 // rows
            wide = jnp.concatenate([src[i * per + j].astype(F32) for j in range(per)], 0)
            scale = lax.rsqrt(jnp.mean(wide * wide, -1, keepdims=True) + 1e-6)
            out = (wide * scale * gain.astype(F32)).astype(BF16)
            for k in range(n_k):
                a_ref[k, pl.ds(16 * i, 16)] = out[:, k * kt : (k + 1) * kt]

    norm_into(xs, gains[0])

    qf[...] = jnp.zeros_like(qf)

    @pl.loop(0, n_q)
    def _(i):
        s = arrived(g_q + i, kt)
        n, k = lax.div(i, n_k), lax.rem(i, n_k)
        qacc[n] = dot(a_ref[k], slot[s, pl.ds(0, kt)]) + jnp.where(k == 0, 0.0, qacc[n])
        issue(g_q + i + n_slots, g_q + n_slots, g_a + n_slots)

    for h in range(heads):
        t = qacc[h * HEAD // W, :, (h * HEAD) % W : (h * HEAD) % W + HEAD].astype(BF16).astype(F32)
        t = t * trig[0] + pltpu.roll(t, HEAD // 2, 1) * trig[1]
        qf[pl.ds(h, batch, stride=hp)] = t.astype(BF16).astype(F32)

    parts_of = 4
    step = cache // parts_of

    def queries(i):
        base = pl.multiple_of(i * 2 * hp, 2 * hp)
        q0, q1 = qf[pl.ds(base, hp)], qf[pl.ds(base + hp, hp)]
        zero = jnp.zeros((hp, HEAD), F32)
        return jnp.concatenate([jnp.concatenate([q0, zero], 1), jnp.concatenate([zero, q1], 1)], 0).astype(BF16)

    def attend(i, score, weigh):
        if score:
            s = arrived(g_a + i, cache)
            q = queries(i)
        if weigh:
            s1 = lax.rem(g_a + i - 1, n_slots)
            old = sc[lax.rem(i + 1, 2)]
            top = jnp.max(old, -1, keepdims=True)
        new, e, total, out = [], [], 0.0, 0.0
        for j in range(parts_of):
            if score:
                new.append(dot_t(q, slot[s, pl.ds(j * step, step), pl.ds(0, 2 * HEAD)]))
            if weigh:
                e.append(jnp.exp((old[:, j * step : (j + 1) * step] - top) * HEAD**-0.5))
                total = total + jnp.sum(e[-1], -1, keepdims=True)
        if weigh:
            inverse = 1.0 / total
            for j in range(parts_of):
                w = (e[j] * inverse).astype(BF16)
                out = out + dot(w, slot[s1, pl.ds(j * step, step), pl.ds(2 * HEAD, 2 * HEAD)])
        if score:
            sc[lax.rem(i, 2)] = jnp.concatenate(new, 1)
        if weigh:
            base = pl.multiple_of((i - 1) * 2 * hp, 2 * hp)
            of[pl.ds(base, hp)] = out[:hp, :HEAD]
            of[pl.ds(base + hp, hp)] = out[hp:, HEAD:]
            issue(g_a + i - 1 + n_slots, g_a + n_slots, g_o + n_slots)

    attend(jnp.int32(0), True, False)

    @pl.loop(1, n_pair)
    def _(i):
        attend(i, True, True)

    attend(jnp.int32(n_pair), False, True)
    for h in range(heads):
        seen[:, pl.ds(h * HEAD, HEAD)] = of[pl.ds(h, batch, stride=hp)].astype(BF16)

    def remote(src, dst, send, recv, device):
        return pltpu.make_async_remote_copy(
            src_ref=src, dst_ref=dst, send_sem=send, recv_sem=recv,
            device_id={"tp": device}, device_id_type=pl.DeviceIdType.MESH,
        )

    def sum_stages(base, width, residual, result):
        cols = pl.ds(0, width)

        def of_tile(t):
            return at(t, width)

        def copy_rs1(t):
            r = lax.rem(base + t, RING)
            return remote(
                send1.at[lax.rem(t, 4), 1 - core, :, :, cols], land1.at[r, :, :, cols], rs1_s.at[r], rs1_r.at[r], partner)

        def copy_rs2(t, d):
            r = lax.rem(base + t, RING)
            return remote(
                send2.at[lax.rem(t, 4), lax.rem(chip + d, chips), :, cols], land2.at[r, d - 1, :, cols],
                rs2_s.at[r, d - 1], rs2_r.at[r, d - 1], peer(d))

        def copy_ag1(t, d):
            r = lax.rem(base + t, RING)
            mine = result.at[me, :, of_tile(t)]
            return remote(mine, mine, ag1_s.at[r, d], ag1_r.at[r, d], peer(d) if d else partner)

        def copy_ag2(t, d):
            r = lax.rem(base + t, RING)
            theirs = result.at[source(d), :, of_tile(t)]
            return remote(theirs, theirs, ag2_s.at[r, d - 1], ag2_r.at[r, d - 1], partner)

        def a(t, term):
            for p in range(n_tp):
                block = term[p * rows : (p + 1) * rows]
                termf[lax.rem(t, 4), p, :, cols] = block
                send1[lax.rem(t, 4), p % 2, p // 2, :, cols] = block.astype(BF16)
            copy_rs1(t).start()

        def b(t):
            copy_rs1(t).wait()
            r, s = lax.rem(base + t, RING), lax.rem(t, 4)
            for c in range(chips):
                both = termf[s, 2 * c + core, :, cols] + land1[r, c, :, cols].astype(F32)
                send2[s, c, :, cols] = both.astype(BF16)
            own[s, :, cols] = termf[s, me, :, cols] + land1[r, chip, :, cols].astype(F32)
            for d in range(1, chips):
                copy_rs2(t, d).start()

        def c(t):
            r, s = lax.rem(base + t, RING), lax.rem(t, 4)
            total = own[s, :, cols]
            for d in range(1, chips):
                copy_rs2(t, d).wait()
                total = total + land2[r, d - 1, :, cols].astype(F32)
            result[me, :, of_tile(t)] = (residual[me, :, of_tile(t)].astype(F32) + total).astype(BF16)
            for d in range(chips):
                copy_ag1(t, d).start()

        def d_(t):
            for d in range(chips):
                copy_ag1(t, d).wait()
            for d in range(1, chips):
                copy_ag2(t, d).start()

        def e(t):
            for d in range(1, chips):
                copy_ag2(t, d).wait()

        return a, b, c, d_, e

    def sum_loop(count, lags, stages, term_of):
        a, *later = stages

        @pl.loop(0, count + lags[-1])
        def _(i):
            for lag, stage in reversed(list(zip(lags, later, strict=True))):

                @pl.when((i >= lag) & (i - lag < count))
                def _():
                    stage(i - lag)

            @pl.when(i < count)
            def _():
                a(i, term_of(i))

    pl.semaphore_wait(barrier, chips)

    def term_o(i):
        s = arrived(g_o + i, 2 * attn)
        lhs = seen[...]
        term = jnp.concatenate([dot(lhs, slot[s, pl.ds(j * attn, attn)]) for j in range(2)], 1)
        issue(g_o + i + n_slots, g_o + n_slots, g_g + n_slots)
        return term

    sum_loop(n_o, (2, 5, 8, 10), sum_stages(0, 2 * W, xs, hs), term_o)
    norm_into(hs, gains[1])

    def gated(gate, up):
        return (jax.nn.silu(gate) * up).astype(BF16)

    @pl.loop(0, n_gu)
    def _(i):
        s = arrived(g_g + i, kt)
        n, r = lax.div(i, 2 * n_k), lax.rem(i, 2 * n_k)
        which, k = lax.div(r, n_k), lax.rem(r, n_k)
        acc[which] = dot(a_ref[k], slot[s, pl.ds(0, kt)]) + jnp.where(k == 0, 0.0, acc[which])
        issue(g_g + i + n_slots, g_g + n_slots, g_r + n_slots)

        @pl.when(r == 2 * n_k - 1)
        def _():
            hidden[:, at(n)] = gated(acc[0], acc[1])

    s = arrived(jnp.int32(g_r), kt)
    both = dot(a_ref[0], slot[s, pl.ds(0, kt), pl.ds(0, 2 * HEAD)]) + dot(a_ref[1], slot[s, pl.ds(0, kt), pl.ds(2 * HEAD, 2 * HEAD)])
    issue(jnp.int32(g_r + n_slots), g_r + n_slots, g_r + n_slots + 1)
    s = arrived(jnp.int32(g_r + 1), kt, 2 * HEAD)
    both = both + dot(a_ref[2], slot[s, pl.ds(0, kt), pl.ds(0, 2 * HEAD)])
    issue(jnp.int32(g_r + 1 + n_slots), g_r + 1 + n_slots, g_r + 2 + n_slots)
    hidden[:, pl.ds(full * W, HEAD)] = gated(both[:, :HEAD], both[:, HEAD:])

    def term_d(i):
        s = arrived(g_d + i, ff)
        term = dot(hidden[...], slot[s, pl.ds(0, ff)])
        issue(g_d + i + n_slots, g_d + n_slots, g_end)
        return term

    sum_loop(n_d, (1, 3, 5, 6), sum_stages(n_o, W, hs, ys), term_d)
    out = pltpu.make_async_copy(ys, o_hbm, out_sem)
    out.start()
    out.wait()


def solution(mesh):
    n_tp = mesh.shape["tp"]

    def step(x, k_cache, v_cache, gain_a, wq, wo, gain_m, w_gate, w_up, w_down):
        batch, d_model = x.shape
        cache, attn, ff = k_cache.shape[1], wq.shape[1], w_down.shape[0]
        rows = batch // n_tp
        n_k = 3
        kt = d_model // n_k
        heads = attn // HEAD
        hp = -(-heads // 8) * 8
        chips = n_tp // 2
        assert ff % W == HEAD and d_model % (2 * W) == 0 and attn % W == 0
        half = HEAD // 2
        angle = jnp.float32(cache - 1) * THETA ** (-jnp.arange(half, dtype=F32) / half)
        cos, sin = jnp.cos(angle)[None], jnp.sin(angle)[None]
        cos2, sin2 = jnp.concatenate([cos, cos], 1), jnp.concatenate([-sin, sin], 1)
        height = max(kt, cache, 2 * attn, ff)
        dma = pltpu.SemaphoreType.DMA
        hbm = pl.BlockSpec(memory_space=pl.ANY)
        y = pl.pallas_call(
            functools.partial(kernel, n_tp),
            out_shape=jax.ShapeDtypeStruct((n_tp, rows, d_model), BF16),
            in_specs=[hbm] * 12,
            out_specs=hbm,
            scratch_shapes=[
                pltpu.VMEM((SLOTS, height, W), BF16),
                dma((SLOTS,)),
                pltpu.VMEM((n_tp, rows, d_model), BF16),
                pltpu.VMEM((n_tp, rows, d_model), BF16),
                pltpu.VMEM((n_tp, rows, d_model), BF16),
                pltpu.VMEM((n_k, batch, kt), BF16),
                pltpu.VMEM((2, 1, d_model), BF16),
                pltpu.VMEM((2, 1, HEAD), F32),
                dma((5,)),
                dma,
                pltpu.VMEM((attn // W, batch, W), F32),
                pltpu.VMEM((batch * hp, HEAD), F32),
                pltpu.VMEM((2, 2 * hp, cache), F32),
                pltpu.VMEM((batch * hp, HEAD), F32),
                pltpu.VMEM((batch, attn), BF16),
                pltpu.VMEM((2, batch, W), F32),
                pltpu.VMEM((batch, ff), BF16),
                pltpu.VMEM((4, n_tp, rows, 2 * W), F32),
                pltpu.VMEM((4, 2, chips, rows, 2 * W), BF16),
                pltpu.VMEM((RING, chips, rows, 2 * W), BF16),
                pltpu.VMEM((4, rows, 2 * W), F32),
                pltpu.VMEM((4, chips, rows, 2 * W), BF16),
                pltpu.VMEM((RING, chips - 1, rows, 2 * W), BF16),
                dma((RING,)),
                dma((RING,)),
                dma((RING, chips - 1)),
                dma((RING, chips - 1)),
                dma((RING, chips)),
                dma((RING, chips)),
                dma((RING, chips - 1)),
                dma((RING, chips - 1)),
            ],
            compiler_params=pltpu.CompilerParams(
                collective_id=0, has_side_effects=True, vmem_limit_bytes=67043328
            ),
            name="layer",
        )(
            x.reshape(n_tp, rows, d_model),
            k_cache.reshape(batch, cache, HEAD), v_cache.reshape(batch, cache, HEAD),
            gain_a[None], wq, wo, gain_m[None], w_gate, w_up, w_down, cos2, sin2,
        )
        return y.reshape(batch, d_model)

    states, cache, columns, rows_of = P("dp", None), P("dp", None, "tp", None), P(None, "tp"), P("tp", None)
    return jax.shard_map(
        step,
        mesh=mesh,
        in_specs=(states, cache, cache, P(None), columns, rows_of, P(None), columns, columns, rows_of),
        out_specs=states,
        check_vma=False,
    )
```

```python
import functools

import jax
import jax.numpy as jnp
import numpy as np
from jax import lax
from jax.experimental import pallas as pl
from jax.experimental.pallas import tpu as pltpu
from jax.sharding import PartitionSpec as P

HEAD = 128
THETA = 10000
W = 512
SLOTS = 11
DEPTH = 4
RING = 12
F32, BF16 = jnp.float32, jnp.bfloat16


def dot(a, b):
    return jnp.dot(a, b, preferred_element_type=F32)


def dot_t(a, b):
    return lax.dot_general(a, b, (((1,), (1,)), ((), ())), preferred_element_type=F32)


def kernel(
    n_tp, x_hbm, k_hbm, v_hbm, ga_hbm, wq, wo, gm_hbm, wg, wu, wd, cos_hbm, sin_hbm, ys,
    slot, slot_sem, xs, hs, a_ref, gains, trig, in_sem, qacc, qf, sc, of, seen, acc, hidden,
    termf, send1, land1, own, send2, land2, rs1_s, rs1_r, rs2_s, rs2_r, ag_s, ag1_r, ag2_r,
):
    d_model = x_hbm.shape[2]
    rows = x_hbm.shape[1]
    batch = x_hbm.shape[0] * rows
    cache = k_hbm.shape[1]
    attn = wq.shape[1]
    heads = attn // HEAD
    hp = qf.shape[0] // batch
    ff = wd.shape[0]
    n_k = a_ref.shape[0]
    kt = a_ref.shape[2]
    chips = n_tp // 2
    n_slots = slot.shape[0]

    me = lax.axis_index("tp")
    chip, core = lax.div(me, 2), lax.rem(me, 2)
    partner = 2 * chip + 1 - core

    def peer(d):
        return 2 * lax.rem(chip + d, chips) + core

    def source(d):
        return 2 * lax.rem(chip - d + chips, chips) + core

    barrier = pltpu.get_barrier_semaphore()
    for other in [partner] + [peer(d) for d in range(1, chips)]:
        pl.semaphore_signal(barrier, inc=1, device_id={"tp": other}, device_id_type=pl.DeviceIdType.MESH)

    n_q, n_pair, n_o = n_k * (attn // W), batch // 2, d_model // (2 * W)
    full = ff // W
    n_gu, n_d = full * 2 * n_k, d_model // W
    g_q, g_a = 0, n_q
    g_o = g_a + n_pair
    g_g = g_o + n_o
    g_r = g_g + n_gu
    g_d = g_r + 2
    g_end = g_d + n_d

    def at(i, step=W):
        return pl.ds(pl.multiple_of(i * step, step), step)

    def lane(i, width=HEAD):
        return pl.ds(i * width, width)

    def start(src, dst, s):
        pltpu.make_async_copy(src, dst, slot_sem.at[s]).start()

    def put_q(i, s):
        start(wq.at[at(lax.rem(i, n_k), kt), at(lax.div(i, n_k))], slot.at[s, pl.ds(0, kt)], s)

    def put_a(i, s):
        for j in range(2):
            start(k_hbm.at[2 * i + j], slot.at[s, pl.ds(0, cache), lane(j)], s)
            start(v_hbm.at[2 * i + j], slot.at[s, pl.ds(0, cache), lane(2 + j)], s)

    def put_o(i, s):
        for j in range(2):
            start(wo.at[:, at(2 * i + j)], slot.at[s, pl.ds(j * attn, attn)], s)

    def put_g(i, s):
        n, r = lax.div(i, 2 * n_k), lax.rem(i, 2 * n_k)

        @pl.when(r < n_k)
        def _():
            start(wg.at[at(r, kt), at(n)], slot.at[s, pl.ds(0, kt)], s)

        @pl.when(r >= n_k)
        def _():
            start(wu.at[at(r - n_k, kt), at(n)], slot.at[s, pl.ds(0, kt)], s)

    def put_r(i, s):
        def piece(w, k, j):
            start(w.at[pl.ds(k * kt, kt), pl.ds(full * W, HEAD)], slot.at[s, pl.ds(0, kt), lane(j)], s)

        @pl.when(i == 0)
        def _():
            for k in range(2):
                piece(wg, k, 2 * k)
                piece(wu, k, 2 * k + 1)

        @pl.when(i == 1)
        def _():
            piece(wg, 2, 0)
            piece(wu, 2, 1)

    def put_d(i, s):
        start(wd.at[:, at(i)], slot.at[s, pl.ds(0, ff)], s)

    parts = [(g_q, g_a, put_q), (g_a, g_o, put_a), (g_o, g_g, put_o), (g_g, g_r, put_g), (g_r, g_d, put_r), (g_d, g_end, put_d)]

    def issue(g, low, high):
        for lo, hi, put in parts:
            if lo < high and low < hi:

                @pl.when((g >= lo) & (g < hi))
                def _():
                    put(g - lo, lax.rem(g, n_slots))

    def arrived(g, height, width=W):
        s = lax.rem(g, n_slots)
        part = slot.at[s, pl.ds(0, height), pl.ds(0, width)]
        pltpu.make_async_copy(part, part, slot_sem.at[s]).wait()
        return s

    inputs = [
        pltpu.make_async_copy(x_hbm, xs, in_sem.at[0]),
        pltpu.make_async_copy(ga_hbm, gains.at[0], in_sem.at[1]),
        pltpu.make_async_copy(gm_hbm, gains.at[1], in_sem.at[2]),
        pltpu.make_async_copy(cos_hbm, trig.at[0], in_sem.at[3]),
        pltpu.make_async_copy(sin_hbm, trig.at[1], in_sem.at[4]),
    ]
    for c in inputs:
        c.start()
    for g in range(2):
        issue(jnp.int32(g), g, g + 1)
    for c in inputs:
        c.wait()
    issue(jnp.int32(2), 2, 3)

    def norm_into(src, gain):
        for i in range(batch // 16):
            per = 16 // rows
            wide = jnp.concatenate([src[i * per + j].astype(F32) for j in range(per)], 0)
            scale = lax.rsqrt(jnp.mean(wide * wide, -1, keepdims=True) + 1e-6)
            for c in range(d_model // HEAD):
                out = (wide[:, c * HEAD : (c + 1) * HEAD] * scale * gain[c : c + 1]).astype(BF16)
                a_ref[c * HEAD // kt, pl.ds(16 * i, 16), pl.ds(c * HEAD % kt, HEAD)] = out

    norm_into(xs, gains[0].astype(F32))

    qf[...] = jnp.zeros_like(qf)

    @pl.loop(0, n_q)
    def _(i):
        s = arrived(g_q + i, kt)
        n, k = lax.div(i, n_k), lax.rem(i, n_k)
        qacc[n] = dot(a_ref[k], slot[s, pl.ds(0, kt)]) + jnp.where(k == 0, 0.0, qacc[n])

        @pl.when(i < n_slots - 3)
        def _():
            issue(2 * i + 3, 0, 2 * n_slots)
            issue(2 * i + 4, 0, 2 * n_slots)

        @pl.when(i >= n_slots - 3)
        def _():
            issue(i + n_slots, n_slots, g_a + n_slots)

    for h in range(heads):
        t = qacc[h * HEAD // W, :, (h * HEAD) % W : (h * HEAD) % W + HEAD].astype(BF16).astype(F32)
        t = t * trig[0] + pltpu.roll(t, HEAD // 2, 1) * trig[1]
        qf[pl.ds(h, batch, stride=hp)] = t.astype(BF16).astype(F32)

    parts_of = 4
    step = cache // parts_of

    def queries(i):
        base = pl.multiple_of(i * 2 * hp, 2 * hp)
        q0, q1 = qf[pl.ds(base, hp)], qf[pl.ds(base + hp, hp)]
        zero = jnp.zeros((hp, HEAD), F32)
        return jnp.concatenate([jnp.concatenate([q0, zero], 1), jnp.concatenate([zero, q1], 1)], 0).astype(BF16)

    def attend(i, score, weigh):
        if score:
            s = arrived(g_a + i, cache)
            q = queries(i)
        if weigh:
            s1 = lax.rem(g_a + i - 1, n_slots)
            old = sc[lax.rem(i + 1, 2)]
            top = jnp.max(old, -1, keepdims=True)
        new, e, total, out = [], [], 0.0, 0.0
        for j in range(parts_of):
            if score:
                new.append(dot_t(q, slot[s, pl.ds(j * step, step), pl.ds(0, 2 * HEAD)]))
            if weigh:
                e.append(jnp.exp((old[:, j * step : (j + 1) * step] - top) * HEAD**-0.5))
                total = total + jnp.sum(e[-1], -1, keepdims=True)
        if weigh:
            inverse = 1.0 / total
            for j in range(parts_of):
                w = (e[j] * inverse).astype(BF16)
                out = out + dot(w, slot[s1, pl.ds(j * step, step), pl.ds(2 * HEAD, 2 * HEAD)])
        if score:
            sc[lax.rem(i, 2)] = jnp.concatenate(new, 1)
        if weigh:
            base = pl.multiple_of((i - 1) * 2 * hp, 2 * hp)
            of[pl.ds(base, hp)] = out[:hp, :HEAD]
            of[pl.ds(base + hp, hp)] = out[hp:, HEAD:]
            issue(g_a + i - 1 + n_slots, g_a + n_slots, g_o + n_slots)

    attend(jnp.int32(0), True, False)

    @pl.loop(1, n_pair)
    def _(i):
        attend(i, True, True)

    attend(jnp.int32(n_pair), False, True)
    for h in range(heads):
        seen[:, pl.ds(h * HEAD, HEAD)] = of[pl.ds(h, batch, stride=hp)].astype(BF16)

    def remote(src, dst, send, recv, device):
        return pltpu.make_async_remote_copy(
            src_ref=src, dst_ref=dst, send_sem=send, recv_sem=recv,
            device_id={"tp": device}, device_id_type=pl.DeviceIdType.MESH,
        )

    def sum_stages(base, width, residual, result):
        cols = pl.ds(0, width)

        def of_tile(t):
            return at(t, width)

        def ring(t):
            return lax.rem(base + t, RING)

        def landed(ref, sem):
            pltpu.make_async_copy(ref, ref, sem).wait()

        def a(t, term):
            s = lax.rem(t, 4)
            for p in range(n_tp):
                block = term[p * rows : (p + 1) * rows]
                termf[s, p, :, cols] = block
                send1[s, p % 2, p // 2, :, cols] = block.astype(BF16)
            remote(send1.at[s, 1 - core, :, :, cols], land1.at[ring(t), :, :, cols], rs1_s.at[s], rs1_r.at[ring(t)], partner).start()

        def b(t):
            r, s, s2 = ring(t), lax.rem(t, 4), lax.rem(t, 8)
            landed(send1.at[s, 0, :, :, cols], rs1_s.at[s])
            landed(land1.at[r, :, :, cols], rs1_r.at[r])
            for c in range(chips):
                both = termf[s, 2 * c + core, :, cols] + land1[r, c, :, cols].astype(F32)
                send2[s2, c, :, cols] = both.astype(BF16)
            own[s2, :, cols] = termf[s, me, :, cols] + land1[r, chip, :, cols].astype(F32)
            for d in range(1, chips):
                src = send2.at[s2, lax.rem(chip + d, chips), :, cols]
                remote(src, land2.at[r, d - 1, :, cols], rs2_s.at[s2], rs2_r.at[r], peer(d)).start()

        def c(t):
            r, s2 = ring(t), lax.rem(t, 8)
            landed(land2.at[r, :, :, cols], rs2_s.at[s2])
            landed(land2.at[r, :, :, cols], rs2_r.at[r])
            total = own[s2, :, cols]
            for d in range(1, chips):
                total = total + land2[r, d - 1, :, cols].astype(F32)
            mine = result.at[me, :, of_tile(t)]
            mine[...] = (residual[me, :, of_tile(t)].astype(F32) + total).astype(BF16)
            for d in range(chips):
                remote(mine, mine, ag_s.at[0], ag1_r.at[r], peer(d) if d else partner).start()

        def d_(t):
            landed(result.at[pl.ds(0, chips), :, of_tile(t)], ag1_r.at[ring(t)])
            for d in range(1, chips):
                theirs = result.at[source(d), :, of_tile(t)]
                remote(theirs, theirs, ag_s.at[1], ag2_r.at[ring(t)], partner).start()

        def e(t):
            landed(result.at[pl.ds(0, chips - 1), :, of_tile(t)], ag2_r.at[ring(t)])

        def end():
            landed(result.at[pl.ds(0, chips)], ag_s.at[0])
            landed(result.at[pl.ds(0, chips - 1)], ag_s.at[1])

        return a, b, c, d_, e, end

    def sum_loop(count, lags, stages, term_of):
        a, *later, end = stages

        @pl.loop(0, count + lags[-1])
        def _(i):
            for lag, stage in reversed(list(zip(lags, later, strict=True))):

                @pl.when((i >= lag) & (i - lag < count))
                def _():
                    stage(i - lag)

            @pl.when(i < count)
            def _():
                a(i, term_of(i))

        end()

    pl.semaphore_wait(barrier, chips)

    def term_o(i):
        s = arrived(g_o + i, 2 * attn)
        lhs = seen[...]
        term = jnp.concatenate([dot(lhs, slot[s, pl.ds(j * attn, attn)]) for j in range(2)], 1)
        issue(g_o + i + n_slots, g_o + n_slots, g_g + n_slots)
        return term

    sum_loop(n_o, (3, 10, 17, 20), sum_stages(0, 2 * W, xs, hs), term_o)
    norm_into(hs, gains[1].astype(F32))

    def gated(gate, up):
        return (jax.nn.silu(gate) * up).astype(BF16)

    @pl.loop(0, n_gu)
    def _(i):
        s = arrived(g_g + i, kt)
        n, r = lax.div(i, 2 * n_k), lax.rem(i, 2 * n_k)
        which, k = lax.div(r, n_k), lax.rem(r, n_k)
        acc[which] = dot(a_ref[k], slot[s, pl.ds(0, kt)]) + jnp.where(k == 0, 0.0, acc[which])
        issue(g_g + i + n_slots, g_g + n_slots, g_r + n_slots)

        @pl.when(r == 2 * n_k - 1)
        def _():
            hidden[:, at(n)] = gated(acc[0], acc[1])

    s = arrived(jnp.int32(g_r), kt)
    both = dot(a_ref[0], slot[s, pl.ds(0, kt), pl.ds(0, 2 * HEAD)]) + dot(a_ref[1], slot[s, pl.ds(0, kt), pl.ds(2 * HEAD, 2 * HEAD)])
    issue(jnp.int32(g_r + n_slots), g_r + n_slots, g_r + n_slots + 1)
    s = arrived(jnp.int32(g_r + 1), kt, 2 * HEAD)
    both = both + dot(a_ref[2], slot[s, pl.ds(0, kt), pl.ds(0, 2 * HEAD)])
    issue(jnp.int32(g_r + 1 + n_slots), g_r + 1 + n_slots, g_r + 2 + n_slots)
    hidden[:, pl.ds(full * W, HEAD)] = gated(both[:, :HEAD], both[:, HEAD:])

    def term_d(i):
        s = arrived(g_d + i, ff)
        term = dot(hidden[...], slot[s, pl.ds(0, ff)])

        @pl.when(i >= n_slots - DEPTH)
        def _():
            issue(g_d + i + DEPTH, g_d + n_slots, g_end)

        return term

    sum_loop(n_d, (2, 7, 12, 14), sum_stages(n_o, W, hs, ys), term_d)


def solution(mesh):
    n_tp = mesh.shape["tp"]

    def step(x, k_cache, v_cache, gain_a, wq, wo, gain_m, w_gate, w_up, w_down):
        batch, d_model = x.shape
        cache, attn, ff = k_cache.shape[1], wq.shape[1], w_down.shape[0]
        rows = batch // n_tp
        n_k = 3
        kt = d_model // n_k
        heads = attn // HEAD
        hp = -(-heads // 8) * 8
        chips = n_tp // 2
        assert ff % W == HEAD and d_model % (2 * W) == 0 and attn % W == 0
        half = HEAD // 2
        angle = np.float32(cache - 1) * np.float32(THETA) ** (-np.arange(half, dtype=np.float32) / np.float32(half))
        cos, sin = np.cos(angle)[None], np.sin(angle)[None]
        cos2, sin2 = np.concatenate([cos, cos], 1), np.concatenate([-sin, sin], 1)
        height = max(kt, cache, 2 * attn, ff)
        dma = pltpu.SemaphoreType.DMA
        hbm = pl.BlockSpec(memory_space=pl.ANY)
        y = pl.pallas_call(
            functools.partial(kernel, n_tp),
            out_shape=pltpu.VMEM((n_tp, rows, d_model), BF16),
            in_specs=[hbm] * 12,
            out_specs=pl.BlockSpec(memory_space=pltpu.VMEM),
            scratch_shapes=[
                pltpu.VMEM((SLOTS, height, W), BF16),
                dma((SLOTS,)),
                pltpu.VMEM((n_tp, rows, d_model), BF16),
                pltpu.VMEM((n_tp, rows, d_model), BF16),
                pltpu.VMEM((n_k, batch, kt), BF16),
                pltpu.VMEM((2, d_model // HEAD, HEAD), BF16),
                pltpu.VMEM((2, 1, HEAD), F32),
                dma((5,)),
                pltpu.VMEM((attn // W, batch, W), F32),
                pltpu.VMEM((batch * hp, HEAD), F32),
                pltpu.VMEM((2, 2 * hp, cache), F32),
                pltpu.VMEM((batch * hp, HEAD), F32),
                pltpu.VMEM((batch, attn), BF16),
                pltpu.VMEM((2, batch, W), F32),
                pltpu.VMEM((batch, ff), BF16),
                pltpu.VMEM((4, n_tp, rows, 2 * W), F32),
                pltpu.VMEM((4, 2, chips, rows, 2 * W), BF16),
                pltpu.VMEM((RING, chips, rows, 2 * W), BF16),
                pltpu.VMEM((8, rows, 2 * W), F32),
                pltpu.VMEM((8, chips, rows, 2 * W), BF16),
                pltpu.VMEM((RING, chips - 1, rows, 2 * W), BF16),
                dma((4,)),
                dma((RING,)),
                dma((8,)),
                dma((RING,)),
                dma((2,)),
                dma((RING,)),
                dma((RING,)),
            ],
            compiler_params=pltpu.CompilerParams(
                collective_id=0, has_side_effects=True, vmem_limit_bytes=64600000
            ),
            name="layer",
        )(
            x.reshape(n_tp, rows, d_model),
            k_cache.reshape(batch, cache, HEAD), v_cache.reshape(batch, cache, HEAD),
            gain_a.reshape(-1, HEAD), wq, wo, gain_m.reshape(-1, HEAD), w_gate, w_up, w_down, cos2, sin2,
        )
        return y.reshape(batch, d_model)

    states, cache, columns, rows_of = P("dp", None), P("dp", None, "tp", None), P(None, "tp"), P("tp", None)
    return jax.shard_map(
        step,
        mesh=mesh,
        in_specs=(states, cache, cache, P(None), columns, rows_of, P(None), columns, columns, rows_of),
        out_specs=states,
        check_vma=False,
    )
```

```python
import functools

import jax
import jax.numpy as jnp
import numpy as np
from jax import lax
from jax.experimental import pallas as pl
from jax.experimental.pallas import tpu as pltpu
from jax.sharding import PartitionSpec as P

HEAD = 128
THETA = 10000
W = 512
SLOTS = 11
DEPTH = 4
WHOLE = 2
RING = 12
F32, BF16 = jnp.float32, jnp.bfloat16


def dot(a, b):
    return jnp.dot(a, b, preferred_element_type=F32)


def dot_t(a, b):
    return lax.dot_general(a, b, (((1,), (1,)), ((), ())), preferred_element_type=F32)


def kernel(
    n_tp, x_hbm, k_hbm, v_hbm, ga_hbm, wq, wo, gm_hbm, wg, wu, wd, cos_hbm, sin_hbm, ys,
    slot, slot_sem, hs, a_ref, gains, trig, in_sem, qacc, qf, sc, seen, acc, hidden,
    termf, send1, land1, own, send2, land2, whole, rs1_s, rs1_r, rs2_s, rs2_r, ag_s, ag1_r, ag2_r,
):
    d_model = x_hbm.shape[2]
    rows = x_hbm.shape[1]
    batch = x_hbm.shape[0] * rows
    cache = k_hbm.shape[1]
    attn = wq.shape[1]
    heads = attn // HEAD
    hp = qf.shape[0] // batch
    ff = wd.shape[0]
    n_k = a_ref.shape[0]
    kt = a_ref.shape[2]
    chips = n_tp // 2
    n_slots = slot.shape[0]

    me = lax.axis_index("tp")
    chip, core = lax.div(me, 2), lax.rem(me, 2)
    partner = 2 * chip + 1 - core

    def peer(d):
        return 2 * lax.rem(chip + d, chips) + core

    def source(d):
        return 2 * lax.rem(chip - d + chips, chips) + core

    barrier = pltpu.get_barrier_semaphore()
    for other in [partner] + [peer(d) for d in range(1, chips)]:
        pl.semaphore_signal(barrier, inc=1, device_id={"tp": other}, device_id_type=pl.DeviceIdType.MESH)

    n_q, n_pair, n_o = n_k * (attn // W), batch // 2, d_model // (2 * W)
    full = ff // W
    n_gu, n_d = full * 2 * n_k, d_model // W
    g_q, g_a = 0, n_q
    g_o = g_a + n_pair
    g_g = g_o + n_o
    g_r = g_g + n_gu
    g_d = g_r + 2
    g_end = g_d + n_d

    def at(i, step=W):
        return pl.ds(pl.multiple_of(i * step, step), step)

    def lane(i, width=HEAD):
        return pl.ds(i * width, width)

    def start(src, dst, s):
        pltpu.make_async_copy(src, dst, slot_sem.at[s]).start()

    def put_q(i, s):
        start(wq.at[at(lax.rem(i, n_k), kt), at(lax.div(i, n_k))], slot.at[s, pl.ds(0, kt)], s)

    def put_a(i, s):
        for j in range(2):
            start(k_hbm.at[2 * i + j], slot.at[s, pl.ds(0, cache), lane(j)], s)
            start(v_hbm.at[2 * i + j], slot.at[s, pl.ds(0, cache), lane(2 + j)], s)

    def put_o(i, s):
        for j in range(2):
            start(wo.at[:, at(2 * i + j)], slot.at[s, pl.ds(j * attn, attn)], s)

    def put_g(i, s):
        n, r = lax.div(i, 2 * n_k), lax.rem(i, 2 * n_k)

        @pl.when(r < n_k)
        def _():
            start(wg.at[at(r, kt), at(n)], slot.at[s, pl.ds(0, kt)], s)

        @pl.when(r >= n_k)
        def _():
            start(wu.at[at(r - n_k, kt), at(n)], slot.at[s, pl.ds(0, kt)], s)

    def put_r(i, s):
        def piece(w, k, j):
            start(w.at[pl.ds(k * kt, kt), pl.ds(full * W, HEAD)], slot.at[s, pl.ds(0, kt), lane(j)], s)

        @pl.when(i == 0)
        def _():
            for k in range(2):
                piece(wg, k, 2 * k)
                piece(wu, k, 2 * k + 1)

        @pl.when(i == 1)
        def _():
            piece(wg, 2, 0)
            piece(wu, 2, 1)

    def put_d(i, s):
        start(wd.at[:, at(i)], slot.at[s, pl.ds(0, ff)], s)

    parts = [(g_q, g_a, put_q), (g_a, g_o, put_a), (g_o, g_g, put_o), (g_g, g_r, put_g), (g_r, g_d, put_r), (g_d, g_end, put_d)]

    def issue(g, low, high):
        for lo, hi, put in parts:
            if lo < high and low < hi:

                @pl.when((g >= lo) & (g < hi))
                def _():
                    put(g - lo, lax.rem(g, n_slots))

    def arrived(g, height, width=W):
        s = lax.rem(g, n_slots)
        part = slot.at[s, pl.ds(0, height), pl.ds(0, width)]
        pltpu.make_async_copy(part, part, slot_sem.at[s]).wait()
        return s

    inputs = [
        pltpu.make_async_copy(x_hbm, hs, in_sem.at[0]),
        pltpu.make_async_copy(ga_hbm, gains.at[0], in_sem.at[1]),
        pltpu.make_async_copy(gm_hbm, gains.at[1], in_sem.at[2]),
        pltpu.make_async_copy(cos_hbm, trig.at[0], in_sem.at[3]),
        pltpu.make_async_copy(sin_hbm, trig.at[1], in_sem.at[4]),
    ]
    for c in inputs:
        c.start()
    for g in range(2):
        issue(jnp.int32(g), g, g + 1)
    for c in inputs:
        c.wait()
    issue(jnp.int32(2), 2, 3)

    def norm_into(src, gain):
        for i in range(batch // 16):
            per = 16 // rows
            wide = jnp.concatenate([src[i * per + j].astype(F32) for j in range(per)], 0)
            scale = lax.rsqrt(jnp.mean(wide * wide, -1, keepdims=True) + 1e-6)
            for c in range(d_model // HEAD):
                out = (wide[:, c * HEAD : (c + 1) * HEAD] * scale * gain[c : c + 1]).astype(BF16)
                a_ref[c * HEAD // kt, pl.ds(16 * i, 16), pl.ds(c * HEAD % kt, HEAD)] = out

    norm_into(hs, gains[0].astype(F32))

    qf[...] = jnp.zeros_like(qf)

    @pl.loop(0, n_q)
    def _(i):
        s = arrived(g_q + i, kt)
        n, k = lax.div(i, n_k), lax.rem(i, n_k)
        qacc[n] = dot(a_ref[k], slot[s, pl.ds(0, kt)]) + jnp.where(k == 0, 0.0, qacc[n])

        @pl.when(i < n_slots - 3)
        def _():
            issue(2 * i + 3, 0, 2 * n_slots)
            issue(2 * i + 4, 0, 2 * n_slots)

        @pl.when(i >= n_slots - 3)
        def _():
            issue(i + n_slots, n_slots, g_a + n_slots)

    for h in range(heads):
        t = qacc[h * HEAD // W, :, (h * HEAD) % W : (h * HEAD) % W + HEAD].astype(BF16).astype(F32)
        t = t * trig[0] + pltpu.roll(t, HEAD // 2, 1) * trig[1]
        qf[pl.ds(h, batch, stride=hp)] = t.astype(BF16).astype(F32)

    parts_of = 4
    step = cache // parts_of

    def queries(i):
        base = pl.multiple_of(i * 2 * hp, 2 * hp)
        q0, q1 = qf[pl.ds(base, hp)], qf[pl.ds(base + hp, hp)]
        zero = jnp.zeros((hp, HEAD), F32)
        return jnp.concatenate([jnp.concatenate([q0, zero], 1), jnp.concatenate([zero, q1], 1)], 0).astype(BF16)

    def attend(i, score, weigh):
        if score:
            s = arrived(g_a + i, cache)
            q = queries(i)
        if weigh:
            s1 = lax.rem(g_a + i - 1, n_slots)
            old = sc[lax.rem(i + 1, 2)]
            top = jnp.max(old, -1, keepdims=True)
        new, e, total, out = [], [], 0.0, 0.0
        for j in range(parts_of):
            if score:
                new.append(dot_t(q, slot[s, pl.ds(j * step, step), pl.ds(0, 2 * HEAD)]))
            if weigh:
                e.append(jnp.exp((old[:, j * step : (j + 1) * step] - top) * HEAD**-0.5))
                total = total + jnp.sum(e[-1], -1, keepdims=True)
        if weigh:
            inverse = 1.0 / total
            for j in range(parts_of):
                w = (e[j] * inverse).astype(BF16)
                out = out + dot(w, slot[s1, pl.ds(j * step, step), pl.ds(2 * HEAD, 2 * HEAD)])
        if score:
            sc[lax.rem(i, 2)] = jnp.concatenate(new, 1)
        if weigh:
            base = pl.multiple_of((i - 1) * 2 * hp, 2 * hp)
            qf[pl.ds(base, hp)] = out[:hp, :HEAD]
            qf[pl.ds(base + hp, hp)] = out[hp:, HEAD:]
            issue(g_a + i - 1 + n_slots, g_a + n_slots, g_o + n_slots)

    attend(jnp.int32(0), True, False)

    @pl.loop(1, n_pair)
    def _(i):
        attend(i, True, True)

    attend(jnp.int32(n_pair), False, True)
    for h in range(heads):
        seen[:, pl.ds(h * HEAD, HEAD)] = qf[pl.ds(h, batch, stride=hp)].astype(BF16)

    def remote(src, dst, send, recv, device):
        return pltpu.make_async_remote_copy(
            src_ref=src, dst_ref=dst, send_sem=send, recv_sem=recv,
            device_id={"tp": device}, device_id_type=pl.DeviceIdType.MESH,
        )

    def sum_stages(base, width, residual, result, count, last):
        cols = pl.ds(0, width)
        early = count - last

        def of_tile(t):
            return at(t, width)

        def ring(t):
            return lax.rem(base + t, RING)

        def landed(ref, sem):
            pltpu.make_async_copy(ref, ref, sem).wait()

        def either(t, usual, final):
            if last:
                pl.when(t < early)(usual)
                pl.when(t >= early)(final)
            else:
                usual()

        def a(t, term):
            s = lax.rem(t, 4)
            for c in range(chips):
                low, high = (term[(2 * c + j) * rows : (2 * c + j + 1) * rows] for j in range(2))
                termf[s, c, :, cols] = jnp.where(core == 0, low, high)
                send1[s, c, :, cols] = jnp.where(core == 0, high, low).astype(BF16)
            remote(send1.at[s, :, :, cols], land1.at[ring(t), :, :, cols], rs1_s.at[s], rs1_r.at[ring(t)], partner).start()

        def b(t):
            r, s, s2 = ring(t), lax.rem(t, 4), lax.rem(t, 8)
            landed(send1.at[s, :, :, cols], rs1_s.at[s])
            landed(land1.at[r, :, :, cols], rs1_r.at[r])
            for c in range(chips):
                both = termf[s, c, :, cols] + land1[r, c, :, cols].astype(F32)
                send2[s2, c, :, cols] = both.astype(BF16)

            def usual():
                own[s2, :, cols] = termf[s, chip, :, cols] + land1[r, chip, :, cols].astype(F32)
                for d in range(1, chips):
                    src = send2.at[s2, lax.rem(chip + d, chips), :, cols]
                    remote(src, land2.at[r, d - 1, :, cols], rs2_s.at[s2], rs2_r.at[r], peer(d)).start()

            def final():
                k = t - early
                for d in range(1, chips):
                    remote(send2.at[s2, :, :, cols], whole.at[k, chip], rs2_s.at[s2], rs2_r.at[r], peer(d)).start()
                whole[k, chip] = send2[s2, :, :, cols]

            either(t, usual, final)

        def c(t):
            r, s2 = ring(t), lax.rem(t, 8)

            def usual():
                landed(land2.at[r, :, :, cols], rs2_s.at[s2])
                landed(land2.at[r, :, :, cols], rs2_r.at[r])
                total = own[s2, :, cols]
                for d in range(1, chips):
                    total = total + land2[r, d - 1, :, cols].astype(F32)
                mine = result.at[me, :, of_tile(t)]
                mine[...] = (residual[me, :, of_tile(t)].astype(F32) + total).astype(BF16)
                for d in range(chips):
                    remote(mine, mine, ag_s.at[0], ag1_r.at[r], peer(d) if d else partner).start()

            def final():
                k = t - early
                landed(whole.at[k, pl.ds(0, chips - 1)], rs2_s.at[s2])
                landed(whole.at[k, pl.ds(0, chips - 1)], rs2_r.at[r])
                for c in range(chips):
                    total = whole[k, 0, c].astype(F32)
                    for q in range(1, chips):
                        total = total + whole[k, q, c].astype(F32)
                    mine = result.at[2 * c + core, :, of_tile(t)]
                    mine[...] = (residual[2 * c + core, :, of_tile(t)].astype(F32) + total).astype(BF16)
                    remote(mine, mine, ag_s.at[2], ag2_r.at[r], partner).start()

            either(t, usual, final)

        def d_(t):
            def usual():
                landed(result.at[pl.ds(0, chips), :, of_tile(t)], ag1_r.at[ring(t)])
                for d in range(1, chips):
                    theirs = result.at[source(d), :, of_tile(t)]
                    remote(theirs, theirs, ag_s.at[1], ag2_r.at[ring(t)], partner).start()

            pl.when(t < early)(usual)

        def e(t):
            def usual():
                landed(result.at[pl.ds(0, chips - 1), :, of_tile(t)], ag2_r.at[ring(t)])

            def final():
                landed(result.at[pl.ds(0, chips), :, of_tile(t)], ag2_r.at[ring(t)])

            either(t, usual, final)

        def end():
            done = pl.ds(0, early * width)
            landed(result.at[pl.ds(0, chips), :, done], ag_s.at[0])
            landed(result.at[pl.ds(0, chips - 1), :, done], ag_s.at[1])
            if last:
                landed(result.at[pl.ds(0, chips), :, pl.ds(0, last * width)], ag_s.at[2])

        return a, b, c, d_, e, end

    def sum_loop(count, lags, stages, term_of):
        a, *later, end = stages

        @pl.loop(0, count + lags[-1])
        def _(i):
            for lag, stage in reversed(list(zip(lags, later, strict=True))):

                @pl.when((i >= lag) & (i - lag < count))
                def _():
                    stage(i - lag)

            @pl.when(i < count)
            def _():
                a(i, term_of(i))

        end()

    pl.semaphore_wait(barrier, chips)

    def term_o(i):
        s = arrived(g_o + i, 2 * attn)
        lhs = seen[...]
        term = jnp.concatenate([dot(lhs, slot[s, pl.ds(j * attn, attn)]) for j in range(2)], 1)
        issue(g_o + i + n_slots, g_o + n_slots, g_g + n_slots)
        return term

    sum_loop(n_o, (3, 9, 15, 18), sum_stages(0, 2 * W, hs, hs, n_o, 0), term_o)
    norm_into(hs, gains[1].astype(F32))

    def gated(gate, up):
        return (jax.nn.silu(gate) * up).astype(BF16)

    @pl.loop(0, n_gu)
    def _(i):
        s = arrived(g_g + i, kt)
        n, r = lax.div(i, 2 * n_k), lax.rem(i, 2 * n_k)
        which, k = lax.div(r, n_k), lax.rem(r, n_k)
        acc[which] = dot(a_ref[k], slot[s, pl.ds(0, kt)]) + jnp.where(k == 0, 0.0, acc[which])
        issue(g_g + i + n_slots, g_g + n_slots, g_r + n_slots)

        @pl.when(r == 2 * n_k - 1)
        def _():
            hidden[:, at(n)] = gated(acc[0], acc[1])

    s = arrived(jnp.int32(g_r), kt)
    both = dot(a_ref[0], slot[s, pl.ds(0, kt), pl.ds(0, 2 * HEAD)]) + dot(a_ref[1], slot[s, pl.ds(0, kt), pl.ds(2 * HEAD, 2 * HEAD)])
    issue(jnp.int32(g_r + n_slots), g_r + n_slots, g_r + n_slots + 1)
    s = arrived(jnp.int32(g_r + 1), kt, 2 * HEAD)
    both = both + dot(a_ref[2], slot[s, pl.ds(0, kt), pl.ds(0, 2 * HEAD)])
    issue(jnp.int32(g_r + 1 + n_slots), g_r + 1 + n_slots, g_r + 2 + n_slots)
    hidden[:, pl.ds(full * W, HEAD)] = gated(both[:, :HEAD], both[:, HEAD:])

    def term_d(i):
        s = arrived(g_d + i, ff)
        term = dot(hidden[...], slot[s, pl.ds(0, ff)])

        @pl.when(i >= n_slots - DEPTH)
        def _():
            issue(g_d + i + DEPTH, g_d + n_slots, g_end)

        return term

    sum_loop(n_d, (2, 5, 8, 10), sum_stages(n_o, W, hs, ys, n_d, WHOLE), term_d)


def solution(mesh):
    n_tp = mesh.shape["tp"]

    def step(x, k_cache, v_cache, gain_a, wq, wo, gain_m, w_gate, w_up, w_down):
        batch, d_model = x.shape
        cache, attn, ff = k_cache.shape[1], wq.shape[1], w_down.shape[0]
        rows = batch // n_tp
        n_k = 3
        kt = d_model // n_k
        heads = attn // HEAD
        hp = -(-heads // 8) * 8
        chips = n_tp // 2
        assert ff % W == HEAD and d_model % (2 * W) == 0 and attn % W == 0
        half = HEAD // 2
        angle = np.float32(cache - 1) * np.float32(THETA) ** (-np.arange(half, dtype=np.float32) / np.float32(half))
        cos, sin = np.cos(angle)[None], np.sin(angle)[None]
        cos2, sin2 = np.concatenate([cos, cos], 1), np.concatenate([-sin, sin], 1)
        height = max(kt, cache, 2 * attn, ff)
        dma = pltpu.SemaphoreType.DMA
        hbm = pl.BlockSpec(memory_space=pl.ANY)
        y = pl.pallas_call(
            functools.partial(kernel, n_tp),
            out_shape=pltpu.VMEM((n_tp, rows, d_model), BF16),
            in_specs=[hbm] * 12,
            out_specs=pl.BlockSpec(memory_space=pltpu.VMEM),
            scratch_shapes=[
                pltpu.VMEM((SLOTS, height, W), BF16),
                dma((SLOTS,)),
                pltpu.VMEM((n_tp, rows, d_model), BF16),
                pltpu.VMEM((n_k, batch, kt), BF16),
                pltpu.VMEM((2, d_model // HEAD, HEAD), BF16),
                pltpu.VMEM((2, 1, HEAD), F32),
                dma((5,)),
                pltpu.VMEM((attn // W, batch, W), F32),
                pltpu.VMEM((batch * hp, HEAD), F32),
                pltpu.VMEM((2, 2 * hp, cache), F32),
                pltpu.VMEM((batch, attn), BF16),
                pltpu.VMEM((2, batch, W), F32),
                pltpu.VMEM((batch, ff), BF16),
                pltpu.VMEM((4, chips, rows, 2 * W), F32),
                pltpu.VMEM((4, chips, rows, 2 * W), BF16),
                pltpu.VMEM((RING, chips, rows, 2 * W), BF16),
                pltpu.VMEM((8, rows, 2 * W), F32),
                pltpu.VMEM((8, chips, rows, 2 * W), BF16),
                pltpu.VMEM((RING, chips - 1, rows, 2 * W), BF16),
                pltpu.VMEM((max(WHOLE, 1), chips, chips, rows, W), BF16),
                dma((4,)),
                dma((RING,)),
                dma((8,)),
                dma((RING,)),
                dma((3,)),
                dma((RING,)),
                dma((RING,)),
            ],
            compiler_params=pltpu.CompilerParams(
                collective_id=0, has_side_effects=True, vmem_limit_bytes=65300000
            ),
            name="layer",
        )(
            x.reshape(n_tp, rows, d_model),
            k_cache.reshape(batch, cache, HEAD), v_cache.reshape(batch, cache, HEAD),
            gain_a.reshape(-1, HEAD), wq, wo, gain_m.reshape(-1, HEAD), w_gate, w_up, w_down, cos2, sin2,
        )
        return y.reshape(batch, d_model)

    states, cache, columns, rows_of = P("dp", None), P("dp", None, "tp", None), P(None, "tp"), P("tp", None)
    return jax.shard_map(
        step,
        mesh=mesh,
        in_specs=(states, cache, cache, P(None), columns, rows_of, P(None), columns, columns, rows_of),
        out_specs=states,
        check_vma=False,
    )
```
